32 devices in a mesh: sub: 2 (over x), vox: 16 (over z, y, core).
Axes of the slice: x: 2, y: 2, z: 4, core: 2. Of those that a mesh axis runs over, the one named last changes fastest.
Arguments:
- observed: float32 [2048, 32768], P('sub', 'vox'), may hold values from -6 to 6
- covariates: float32 [2048, 64], P('sub'), may hold values from -0.26516504 to 0.26516504
- voxel_mask: int32 [32768], P('vox'), may hold values 0 or 1
- tau_index: int32 [1], replicated, may hold values from 2 to 18
Outputs:
- coefficients: float32 [64, 32768], P(None, 'vox')
- split_residual: float32 [2048, 32768], P('sub', 'vox')
The draws below stay inside these ranges and needn't reach their ends.
All inputs are finite; a program needn't handle non-finite values. Where the reference program divides by a largest or mean magnitude, that divisor is 1e-20 or more. No bound on the sum of `voxel_mask` on one device may be relied on, other than what follows from the above.
Results may differ from the reference program's by a relative error of at most 0.0001.
Values sent between devices are 32-bit elements; how exact they have to be, the bound alone decides.
No kernel may reach another device: no remote copies, remote signals or barrier semaphores. Data moves between devices by JAX's collectives and lax.ppermute only.
A program may use at most 128 MiB of HBM per device.

```python
import jax
import jax.numpy as jnp
from jax import lax

COVARS = 64
PX = 8
PY = 8
GZ = 32
NPY = 8
ITERS = 3
QUANT = 20
NPX = 2
GX = 16
GY = 64
VOXELS = 32768
SUBJECTS = 2048


def draw_covariates(key, part):
    scale_key = jax.random.fold_in(key, 11)
    value_key = jax.random.fold_in(key, 12)
    scales = jnp.exp(jax.random.uniform(scale_key, (COVARS,), jnp.float32, jnp.log(0.3), jnp.log(3.0)))
    values = jnp.clip(jax.random.normal(value_key, (SUBJECTS, COVARS), jnp.float32), -4.0, 4.0)
    return values * scales[None, :] / jnp.sqrt(jnp.float32(SUBJECTS))


def plant(array, rng, least, largest):
    shape = array.shape
    index_at = [jax.random.randint(jax.random.fold_in(rng, axis), (), 0, shape[axis]) for axis in range(len(shape))]
    array = array.at[tuple(index_at)].set(least)
    longest = shape.index(max(shape))
    index_at[longest] = (index_at[longest] + 1) % shape[longest]
    return array.at[tuple(index_at)].set(largest)


def shard_levels(own_key, shape, split, low, largest):
    def one(position, shards_of):
        draws = jax.random.uniform(jax.random.fold_in(jax.random.fold_in(own_key, 6), position), (shards_of,), jnp.float32, low / len(split), largest / len(split))
        return jnp.repeat(jnp.exp(draws), shape[position] // shards_of).reshape((-1,) + (1,) * (len(shape) - position - 1))

    level = one(*split[0])
    for cut in split[1:]:
        level = level * one(*cut)
    return level


def gaussian(own_key, shape, scale, most, cuts=(), held_as=jnp.bfloat16):
    gain = shard_levels(own_key, shape, cuts, -0.22, 0.18) if cuts else 1.0
    drawn = jax.random.normal(own_key, shape, jnp.float32) * scale * gain
    return jnp.minimum(jnp.maximum(drawn, -most), most).astype(held_as)


def setup_inputs(seed: int = 0) -> dict:
    splits = jax.random.split(jax.random.key(seed), 5)
    return {
        "observed": gaussian(splits[0], (SUBJECTS, VOXELS), 1.0, 6.0, ((0, 2), (1, 16)), jnp.float32),
        "covariates": draw_covariates(jax.random.fold_in(splits[4], 71), 0),
        "voxel_mask": plant((jax.random.randint(splits[2], (VOXELS,), 0, 4) < 3).astype(jnp.int32), jax.random.fold_in(splits[2], 1), 0, 1),
        "tau_index": jax.random.randint(splits[3], (1,), 2, 19).astype(jnp.int32),
    }


penalty_fit = 1.0
penalty_tv = 1.0
tv_weight = 0.05
huber_width = 0.02


def to_grid(flat):
    leading = flat.shape[:-1]
    lead_rank = len(leading)
    blocks = flat.reshape(leading + (NPX * NPY, PX * PY * GZ))
    blocks = jnp.roll(blocks, NPY // 2, axis=lead_rank)
    axis_order = tuple(range(lead_rank)) + (lead_rank, lead_rank + 2, lead_rank + 1, lead_rank + 3, lead_rank + 4)
    pieces = blocks.reshape(leading + (NPX, NPY, PX, PY, GZ)).transpose(axis_order)
    return pieces.reshape(leading + (GX, GY, GZ))


def to_flat(volume):
    leading = volume.shape[:-3]
    lead_rank = len(leading)
    axis_order = tuple(range(lead_rank)) + (lead_rank, lead_rank + 2, lead_rank + 1, lead_rank + 3, lead_rank + 4)
    pieces = volume.reshape(leading + (NPX, PX, NPY, PY, GZ)).transpose(axis_order)
    blocks = pieces.reshape(leading + (NPX * NPY, PX * PY * GZ))
    blocks = jnp.roll(blocks, -(NPY // 2), axis=lead_rank)
    return blocks.reshape(leading + (VOXELS,))


def shift_next(field, along):
    extent = field.shape[along]
    later = lax.slice_in_dim(field, 1, extent, axis=along)
    padding = jnp.zeros_like(lax.slice_in_dim(field, 0, 1, axis=along))
    return jnp.concatenate([later, padding], along)


def shift_prev(field, along):
    extent = field.shape[along]
    earlier = lax.slice_in_dim(field, 0, extent - 1, axis=along)
    padding = jnp.zeros_like(lax.slice_in_dim(field, 0, 1, axis=along))
    return jnp.concatenate([padding, earlier], along)


def forward(volume):
    results = [jnp.roll(volume, -1, axis=1) - volume]
    for along in (2, 3):
        places = lax.broadcasted_iota(jnp.int32, volume.shape, along)
        inner = (places < volume.shape[along] - 1).astype(volume.dtype)
        results.append(inner * (shift_next(volume, along) - volume))
    return jnp.stack(results)


def adjoint(dual_tv):
    summed = jnp.roll(dual_tv[0], 1, axis=1) - dual_tv[0]
    summed = summed + (shift_prev(dual_tv[1], 2) - dual_tv[1])
    summed = summed + (shift_prev(dual_tv[2], 3) - dual_tv[2])
    return summed


def huber_prox(target):
    clip_bound = tv_weight / penalty_tv
    return target - jnp.clip(target * (clip_bound / (huber_width + clip_bound)), -clip_bound, clip_bound)


def first_sums(observed, covariates, masked):
    highest = lax.Precision.HIGHEST
    block = PX * PY * GZ

    def one_block(index, summed):
        start = (index * block).astype(jnp.int32)
        rows = lax.dynamic_slice_in_dim(observed, start, block, 1)
        mask_block = lax.dynamic_slice_in_dim(masked, start, block, 0)[None, :]
        term = jnp.dot(covariates.T, mask_block * rows, precision=highest)
        return lax.dynamic_update_slice_in_dim(summed, term, start, 1)

    initial = jnp.zeros((COVARS, VOXELS), jnp.float32)
    return lax.fori_loop(0, VOXELS // block, one_block, initial)


def state_pass(observed, covariates, masked, flat_coeffs, split_res, scaled_dual, summed, quantile, want_next):
    highest = lax.Precision.HIGHEST
    block = PX * PY * GZ

    def one_block(index, carry):
        split_res, scaled_dual, summed = carry
        start = (index * block).astype(jnp.int32)
        rows = lax.dynamic_slice_in_dim(observed, start, block, 1)
        mask_block = lax.dynamic_slice_in_dim(masked, start, block, 0)[None, :]
        coef_block = lax.dynamic_slice_in_dim(flat_coeffs, start, block, 1)
        fitted = rows - jnp.dot(covariates, coef_block, precision=highest)
        old_dual = lax.dynamic_slice_in_dim(scaled_dual, start, block, 1)
        target = fitted + old_dual
        new_split = mask_block * (target - jnp.clip(target, (quantile - 1.0) / penalty_fit, quantile / penalty_fit))
        new_dual = old_dual + mask_block * (fitted - new_split)
        split_res = lax.dynamic_update_slice_in_dim(split_res, new_split, start, 1)
        scaled_dual = lax.dynamic_update_slice_in_dim(scaled_dual, new_dual, start, 1)
        if want_next:
            misfit = mask_block * (fitted - new_split + new_dual)
            term = jnp.dot(covariates.T, misfit, precision=highest)
            summed = lax.dynamic_update_slice_in_dim(summed, term, start, 1)
        return split_res, scaled_dual, summed

    return lax.fori_loop(0, VOXELS // block, one_block, (split_res, scaled_dual, summed))


def reference(observed, covariates, voxel_mask, tau_index):
    highest = lax.Precision.HIGHEST
    quantile = tau_index[0].astype(jnp.float32) / QUANT
    gram_matrix = jnp.dot(covariates.T, covariates, precision=highest)
    row_bound = jnp.max(jnp.sum(jnp.abs(gram_matrix), axis=1))
    step_size = 1.0 / (penalty_fit * row_bound + 12.0 * penalty_tv)
    masked = voxel_mask.astype(jnp.float32)
    coeffs = jnp.zeros((COVARS, GX, GY, GZ), jnp.float32)
    differences = jnp.zeros((3, COVARS, GX, GY, GZ), jnp.float32)
    split_tv = jnp.zeros((3, COVARS, GX, GY, GZ), jnp.float32)
    tv_dual = jnp.zeros((3, COVARS, GX, GY, GZ), jnp.float32)
    split_res = jnp.zeros_like(observed)
    scaled_dual = jnp.zeros_like(observed)
    summed_flat = first_sums(observed, covariates, masked)
    for iteration in range(ITERS):
        dual_tv = differences - split_tv + tv_dual
        coeffs = coeffs - step_size * (-penalty_fit * to_grid(summed_flat) + penalty_tv * adjoint(dual_tv))
        flat_coeffs = to_flat(coeffs)
        split_res, scaled_dual, summed_flat = state_pass(observed, covariates, masked, flat_coeffs, split_res, scaled_dual, summed_flat, quantile, iteration + 1 < ITERS)
        differences = forward(coeffs)
        target_tv = differences + tv_dual
        split_tv = huber_prox(target_tv)
        tv_dual = tv_dual + differences - split_tv
    return to_flat(coeffs), split_res
```

```python
import functools

import jax
import jax.numpy as jnp
from jax import lax
from jax.experimental import pallas as pl
from jax.experimental.pallas import tpu as pltpu
from jax.sharding import PartitionSpec as P

COVARS = 64
PX = 8
PY = 8
GZ = 32
NPY = 8
QUANT = 20
LANES = 128

LAYER = PY * GZ
HALVES = LAYER // LANES
PER_TILE = LANES // GZ
CHUNKS = ((PX - 1, 0), (1, 2), (3, 4), (5, 6))
ROWS = 256

penalty_fit = 1.0
penalty_tv = 1.0
tv_weight = 0.05
huber_width = 0.02
CLIP_TV = tv_weight / penalty_tv
KAPPA = CLIP_TV / (huber_width + CLIP_TV)

F32 = jnp.float32
BF16 = jnp.bfloat16

VMEM = pl.BlockSpec(memory_space=pltpu.VMEM)
SMEM = pl.BlockSpec(memory_space=pltpu.SMEM)
ANY = pl.BlockSpec(memory_space=pl.ANY)


def moved(block, axis, distance):
    size = lax.axis_size(axis)
    route = [((i - distance) % size, i) for i in range(size)]
    return lax.ppermute(block, axis, route)


def others_sum(block, axis):
    received = moved(block, axis, 1)
    for distance in range(2, lax.axis_size(axis)):
        received = received + moved(block, axis, distance)
    return received


def windows(layers):
    runs = []
    for place, layer in enumerate(layers):
        if runs and runs[-1][0] + runs[-1][2] == layer * LAYER:
            runs[-1][2] += LAYER
        else:
            runs.append([layer * LAYER, place * LAYER, LAYER])
    return runs


def dot(a, b):
    return jnp.dot(a, b, preferred_element_type=F32)


def halves(value):
    high = value.astype(BF16)
    return high, (value - high.astype(F32)).astype(BF16)


def columns_of(ref, layers):
    return jnp.concatenate([ref[:, first : first + width] for first, _, width in windows(layers)], 1)


def copies(source, target, sems, layers, into_chunk):
    plan = []
    for block in range(source.shape[0] // ROWS):
        rows = pl.ds(block * ROWS, ROWS)
        row = []
        for number, (first, place, width) in enumerate(windows(layers)):
            far, near = (rows, pl.ds(first, width)), (rows, pl.ds(place, width))
            src, dst = (far, near) if into_chunk else (near, far)
            row.append(pltpu.make_async_copy(source.at[src], target.at[dst], sems.at[block, number]))
        plan.append(row)
    return plan


def start(row):
    for copy in row:
        copy.start()


def wait(row):
    for copy in row:
        copy.wait()


def call(kernel, out_shape, in_specs, out_specs, scratch, flops, args, aliases=None):
    return pl.pallas_call(
        kernel,
        out_shape=out_shape,
        in_specs=in_specs,
        out_specs=out_specs,
        scratch_shapes=scratch,
        input_output_aliases=aliases or {},
        cost_estimate=pl.CostEstimate(flops=flops, bytes_accessed=4 << 20, transcendentals=0),
        compiler_params=pltpu.CompilerParams(vmem_limit_bytes=24 << 20),
    )(*args)


def sds(*shape, dtype=F32):
    return jax.ShapeDtypeStruct(shape, dtype)


def first_kernel(layers, prepare, *refs):
    if prepare:
        obs, cov, part, xe, xt, ybuf, sems = refs
    else:
        obs, xt, part, ybuf, sems = refs
    loads = copies(obs, ybuf, sems, layers, True)
    for row in loads:
        start(row)
    if prepare:
        x = cov[...]
        high = x.astype(BF16).astype(F32)
        low = (x - high).astype(BF16).astype(F32)
        xe[...] = jnp.concatenate([high, high, low, low], 1).astype(BF16)
        both = jnp.concatenate([high, low], 1)
        xt[...] = both.T.astype(BF16)
        gram = dot(xt[...], both.astype(BF16))
        gram = gram[:COVARS] + gram[COVARS:]
        gram = gram + pltpu.roll(gram, COVARS, 1)
        part[:, len(layers) * LAYER :] = gram
    total = jnp.zeros((2 * COVARS, len(layers) * LAYER), F32)
    for block, row in enumerate(loads):
        wait(row)
        rows = slice(block * ROWS, (block + 1) * ROWS)
        high, low = halves(ybuf[rows, :])
        total = total + dot(xt[:, rows], high) + dot(xt[:, rows], low)
    part[:, : len(layers) * LAYER] = total[:COVARS] + total[COVARS:]


def first_stage(layers, obs, cov, xt):
    rows, width = obs.shape[0], len(layers) * LAYER
    scratch = [
        pltpu.VMEM((rows, width), F32),
        pltpu.SemaphoreType.DMA((rows // ROWS, len(windows(layers)))),
    ]
    flops = 2 * rows * 2 * COVARS * 2 * width
    if xt is None:
        out = (sds(COVARS, width + LANES), sds(rows, 4 * COVARS, dtype=BF16), sds(2 * COVARS, rows, dtype=BF16))
        return call(
            functools.partial(first_kernel, layers, True), out, [ANY, VMEM], (VMEM,) * 3, scratch, flops, (obs, cov)
        )
    out = sds(COVARS, width)
    return call(functools.partial(first_kernel, layers, False), out, [ANY, VMEM], VMEM, scratch, flops, (obs, xt))


def packed_rows(chunks, lane):
    at = lax.broadcasted_iota(jnp.int32, (COVARS, LANES), 1) // GZ
    tiles = []
    for tile in range(PX // PER_TILE):
        built = None
        for place in range(PER_TILE):
            layer = tile * PER_TILE + place
            number = next(n for n, layers in enumerate(CHUNKS) if layer in layers)
            first = CHUNKS[number].index(layer) * LAYER + lane * GZ
            base = first // LANES * LANES
            piece = chunks[number][:, base : base + LANES]
            shift = (place * GZ - (first - base)) % LANES
            piece = pltpu.roll(piece, shift, 1) if shift else piece
            built = piece if built is None else jnp.where(at == place, piece, built)
        tiles.append(built)
    return jnp.concatenate(tiles, 1)


def step_kernel(layers, stage, opening, closing, *refs):
    refs = list(refs)
    take = lambda: refs.pop(0)
    tau, mask, own, got = take(), take(), take(), take()
    eta_in = None if opening else take()
    base, grad = (take(), take()) if stage > 1 else (None, None)
    xe, xt, obs = take(), take(), take()
    earlier = [take() for _ in range(len(CHUNKS) - 1)] if closing else []
    coef, part = take(), take()
    eta_out = take() if opening else None
    carry, state = (take(), take()) if stage == 2 else (None, None)
    heads, tails = (take(), take()) if closing else (None, None)
    bext, ybuf, sems = take(), take(), take()
    bold, zbuf, zsems = (take(), take(), take()) if stage == 2 else (None, None, None)

    width = len(layers) * LAYER
    loads = copies(obs, ybuf, sems, layers, True)
    for row in loads:
        start(row)
    if opening:
        gram = jnp.abs(own[:, width:] + got[:, width:])
        first_half = lax.broadcasted_iota(jnp.int32, gram.shape, 1) < COVARS
        bound = jnp.max(jnp.sum(jnp.where(first_half, gram, 0.0), 0, keepdims=True), 1, keepdims=True)
        eta = 1.0 / (penalty_fit * bound + 12.0 * penalty_tv)
        eta_out[...] = jnp.broadcast_to(eta, eta_out.shape)
    else:
        eta = eta_in[0:1, 0:1]
    scale = eta * columns_of(mask, layers).astype(F32)
    quantile = jnp.full((1, width), tau[0], jnp.int32).astype(F32) / QUANT
    lower, upper = (quantile - 1.0) / penalty_fit, quantile / penalty_fit

    summed = penalty_fit * (own[:, :width] + got[:, :width])
    if stage == 1:
        now = scale * summed
    else:
        old = base[...]
        now = old + (2.0 * scale) * summed - (eta * penalty_tv) * grad[...]
        carry[...] = now - scale * summed
        high, low = halves(old)
        bold[...] = jnp.concatenate([high, low, high, low], 0)
    coef[...] = now
    high, low = halves(now)
    bext[...] = jnp.concatenate([high, low, high, low], 0)
    if closing:
        order = earlier + [coef]
        heads[...] = packed_rows(order, 0)
        tails[...] = packed_rows(order, PY - 1)

    total = jnp.zeros((2 * COVARS, width), F32)
    stores = copies(zbuf, state, zsems, ((0, 1) if len(layers) == 2 else tuple(range(len(layers)))), False) if stage == 2 else []
    for block, row in enumerate(loads):
        rows = slice(block * ROWS, (block + 1) * ROWS)
        fit = dot(xe[rows, :], bext[...])
        if stage == 2:
            fit_old = dot(xe[rows, :], bold[...])
        wait(row)
        y = ybuf[rows, :]
        target = y - fit
        if stage == 2:
            target = target + jnp.clip(y - fit_old, lower, upper)
        dual = jnp.clip(target, lower, upper)
        if stage == 2:
            zbuf[rows, :] = y + dual
            start(stores[block])
        high, low = halves(dual)
        total = total + dot(xt[:, rows], high) + dot(xt[:, rows], low)
    part[...] = total[:COVARS] + total[COVARS:]
    for row in stores:
        wait(row)


def step_stage(layers, stage, tau, mask, own, got, eta, base, grad, xe, xt, obs, earlier):
    rows, width = obs.shape[0], len(layers) * LAYER
    opening, closing = eta is None, earlier is not None
    args, specs = [tau, mask, own, got], [SMEM, VMEM, VMEM, VMEM]
    if not opening:
        args, specs = args + [eta], specs + [VMEM]
    if stage > 1:
        args, specs = args + [base, grad], specs + [VMEM, VMEM]
    args, specs = args + [xe, xt, obs], specs + [VMEM, VMEM, ANY]
    if closing:
        args, specs = args + earlier, specs + [VMEM] * len(earlier)
    out, out_specs = [sds(COVARS, width)] * 2, [VMEM] * 2
    if opening:
        out, out_specs = out + [sds(8, LANES)], out_specs + [VMEM]
    if stage == 2:
        out, out_specs = out + [sds(COVARS, width), sds(rows, width)], out_specs + [VMEM, ANY]
    if closing:
        out, out_specs = out + [sds(COVARS, PX * GZ)] * 2, out_specs + [VMEM] * 2
    scratch = [
        pltpu.VMEM((4 * COVARS, width), BF16),
        pltpu.VMEM((rows, width), F32),
        pltpu.SemaphoreType.DMA((rows // ROWS, len(windows(layers)))),
    ]
    if stage == 2:
        scratch += [
            pltpu.VMEM((4 * COVARS, width), BF16),
            pltpu.VMEM((rows, width), F32),
            pltpu.SemaphoreType.DMA((rows // ROWS, 1)),
        ]
    kernel = functools.partial(step_kernel, layers, stage, opening, closing)
    flops = 2 * rows * width * (2 * 2 * COVARS + 4 * COVARS * stage)
    return call(kernel, tuple(out), specs, tuple(out_specs), scratch, flops, args)


def tv_kernel(passes, npx_ends, edge, *refs):
    refs = list(refs)
    fields = []
    for _ in range(passes):
        chunks = [refs.pop(0) for _ in CHUNKS]
        from_left, from_right = refs.pop(0), refs.pop(0)
        heads, tails, before, after = [refs.pop(0) for _ in range(4)]
        fields.append((chunks, from_left, from_right, heads, tails, before, after))
    outs = refs
    place_of = {layer: (n, c.index(layer)) for n, c in enumerate(CHUNKS) for layer in c}
    lane = lax.broadcasted_iota(jnp.int32, (8, LANES), 1)
    first_y = edge[0] > 0
    last_y = edge[1] > 0

    def one_group(group, carry):
        rows = pl.ds(pl.multiple_of(group * 8, 8), 8)
        keep_y = jnp.where(edge[1] > 0, 0.0, 1.0)
        keep_prev = jnp.where(edge[0] > 0, 0.0, 1.0)

        def tile(field, layer, half):
            chunks, from_left, from_right = field[:3]
            if layer < 0:
                return from_left[rows, half * LANES : (half + 1) * LANES]
            if layer == PX:
                return from_right[rows, LAYER + half * LANES : LAYER + (half + 1) * LANES]
            number, place = place_of[layer]
            first = place * LAYER + half * LANES
            return chunks[number][rows, first : first + LANES]

        def dual_of(steps):
            q = None
            for step in steps:
                before = q
                q = jnp.clip((step if q is None else step + q) * KAPPA, -CLIP_TV, CLIP_TV)
            return 2.0 * q if before is None else 2.0 * q - before

        def dual_x(layer, half):
            return dual_of([tile(f, layer + 1, half) - tile(f, layer, half) for f in fields])

        def dual_z(layer, half):
            steps = []
            for f in fields:
                now = tile(f, layer, half)
                steps.append(jnp.where(lane % GZ == GZ - 1, 0.0, pltpu.roll(now, LANES - 1, 1) - now))
            return dual_of(steps)

        def dual_y(layer, half):
            steps = []
            group_at, spot = layer // PER_TILE, layer % PER_TILE
            for f in fields:
                now = tile(f, layer, half)
                if half + 1 < HALVES:
                    after = pltpu.roll(tile(f, layer, half + 1), LANES - GZ, 1)
                else:
                    after = f[6][rows, group_at * LANES : (group_at + 1) * LANES]
                    shift = (LANES - GZ - spot * GZ) % LANES
                    after = pltpu.roll(after, shift, 1) if shift else after
                following = jnp.where(lane < LANES - GZ, pltpu.roll(now, LANES - GZ, 1), after)
                step = following - now
                if half + 1 == HALVES:
                    step = step * jnp.where(lane < LANES - GZ, 1.0, keep_y)
                steps.append(step)
            return dual_of(steps)

        edge_duals = []
        for group_at in range(PX // PER_TILE):
            at = slice(group_at * LANES, (group_at + 1) * LANES)
            edge_duals.append(dual_of([(f[3][rows, at] - f[5][rows, at]) * keep_prev for f in fields]))

        before_x = [dual_x(-1, half) for half in range(HALVES)]
        for layer in range(PX):
            number, place = place_of[layer]
            group_at, spot = layer // PER_TILE, layer % PER_TILE
            shift = (LANES - spot * GZ) % LANES
            before_y = pltpu.roll(edge_duals[group_at], shift, 1) if shift else edge_duals[group_at]
            for half in range(HALVES):
                x_now = dual_x(layer, half)
                y_now = dual_y(layer, half)
                z_now = dual_z(layer, half)
                rolled = pltpu.roll(y_now, GZ, 1)
                summed = before_x[half] - x_now
                summed = summed + (jnp.where(lane < GZ, before_y, rolled) - y_now)
                summed = summed + (pltpu.roll(z_now, 1, 1) - z_now)
                first = place * LAYER + half * LANES
                outs[number][rows, first : first + LANES] = summed
                before_x[half] = x_now
                before_y = rolled
        return carry

    lax.fori_loop(0, COVARS // 8, one_group, 0)


def tv_stage(edge, fields):
    args, specs = [edge], [SMEM]
    for chunks, *rest in fields:
        args += list(chunks) + rest
        specs += [VMEM] * (len(chunks) + len(rest))
    out = tuple(sds(COVARS, len(c) * LAYER) for c in CHUNKS)

    def kernel(edge_ref, *refs):
        tv_kernel(len(fields), None, edge_ref, *refs)

    flops = len(fields) * 60 * COVARS * PX * LAYER * 64
    return call(kernel, out, specs, (VMEM,) * len(out), [], flops, args)


def last_kernel(layers, first, *refs):
    refs = list(refs)
    take = lambda: refs.pop(0)
    tau, mask, own, got, eta, base, grad, xe, state = [take() for _ in range(9)]
    if not first:
        take(), take()
    coef_out, res_out, bext, zbuf, zsems, rbuf, rsems, cbuf, csems = [take() for _ in range(9)]
    width = len(layers) * LAYER
    loads = copies(state, zbuf, zsems, tuple(range(len(layers))), True)
    for row in loads:
        start(row)
    kept = columns_of(mask, layers).astype(F32)
    quantile = jnp.full((1, width), tau[0], jnp.int32).astype(F32) / QUANT
    lower, upper = (quantile - 1.0) / penalty_fit, quantile / penalty_fit
    step = eta[0:1, 0:1]
    summed = penalty_fit * (own[...] + got[...])
    now = base[...] + (2.0 * step * kept) * summed - (step * penalty_tv) * grad[...]
    cbuf[...] = now
    coef_stores = []
    for number, (at, place, span) in enumerate(windows(layers)):
        coef_stores.append(
            pltpu.make_async_copy(cbuf.at[:, pl.ds(place, span)], coef_out.at[:, pl.ds(at, span)], csems.at[number])
        )
    start(coef_stores)
    high, low = halves(now)
    bext[...] = jnp.concatenate([high, low, high, low], 0)
    stores = copies(rbuf, res_out, rsems, layers, False)
    for block, row in enumerate(loads):
        rows = slice(block * ROWS, (block + 1) * ROWS)
        fit = dot(xe[rows, :], bext[...])
        wait(row)
        target = zbuf[rows, :] - fit
        rbuf[rows, :] = kept * (target - jnp.clip(target, lower, upper))
        start(stores[block])
    wait(coef_stores)
    for row in stores:
        wait(row)


def last_stage(layers, pencil, tau, mask, own, got, eta, base, grad, xe, state, outs):
    rows, width = state.shape
    args = [tau, mask, own, got, eta, base, grad, xe, state]
    specs = [SMEM] + [VMEM] * 7 + [ANY]
    aliases = {}
    if outs is not None:
        aliases = {len(args): 0, len(args) + 1: 1}
        args, specs = args + list(outs), specs + [ANY, ANY]
    runs = len(windows(layers))
    scratch = [
        pltpu.VMEM((4 * COVARS, width), BF16),
        pltpu.VMEM((rows, width), F32),
        pltpu.SemaphoreType.DMA((rows // ROWS, 1)),
        pltpu.VMEM((rows, width), F32),
        pltpu.SemaphoreType.DMA((rows // ROWS, runs)),
        pltpu.VMEM((COVARS, width), F32),
        pltpu.SemaphoreType.DMA((runs,)),
    ]
    out = (sds(COVARS, pencil), sds(rows, pencil))
    kernel = functools.partial(last_kernel, layers, outs is None)
    flops = 2 * rows * width * 4 * COVARS * 2
    return call(kernel, out, specs, (ANY, ANY), scratch, flops, args, aliases)


def neighbours_x(chunk):
    size = lax.axis_size("vox")
    before = moved(chunk, "vox", NPY)
    after = before if (2 * NPY) % size == 0 else moved(chunk, "vox", -NPY)
    return before, after


def per_device(observed, covariates, voxel_mask, tau_index):
    pencils = lax.axis_size("vox")
    pencil_y = (lax.axis_index("vox") + NPY // 2) % pencils % NPY
    edge = jnp.stack([(pencil_y == 0).astype(jnp.int32), (pencil_y == NPY - 1).astype(jnp.int32)])
    mask = voxel_mask.reshape(1, -1)
    count = len(CHUNKS)

    parts, xe, xt = [], None, None
    for number, layers in enumerate(CHUNKS):
        if number == 0:
            part, xe, xt = first_stage(layers, observed, covariates, None)
        else:
            part = first_stage(layers, observed, None, xt)
        parts.append((part, others_sum(part, "sub")))

    eta, base, grad, states, fields = None, None, None, None, []
    for stage in (1, 2):
        coefs, carries, new_parts, new_states = [], [], [], []
        for number, layers in enumerate(CHUNKS):
            own, got = parts[number]
            earlier = list(coefs) if number == count - 1 else None
            results = list(
                step_stage(
                    layers, stage, tau_index, mask, own, got, eta,
                    base[number] if base else None, grad[number] if grad else None, xe, xt, observed, earlier,
                )
            )
            coefs.append(results.pop(0))
            part = results.pop(0)
            new_parts.append((part, others_sum(part, "sub")))
            if eta is None:
                eta = results.pop(0)
            if stage == 2:
                carries.append(results.pop(0))
                new_states.append(results.pop(0))
            if number == 0:
                from_left, from_right = neighbours_x(coefs[0])
            if earlier is not None:
                heads, tails = results
        before, after = moved(tails, "vox", 1), moved(heads, "vox", -1)
        fields.append((coefs, from_left, from_right, heads, tails, before, after))
        grad = tv_stage(edge, fields)
        base = coefs if stage == 1 else carries
        parts, states = new_parts, new_states

    outs = None
    for number, layers in enumerate(CHUNKS):
        own, got = parts[number]
        outs = last_stage(
            layers, observed.shape[1], tau_index, mask, own, got, eta, base[number], grad[number], xe, states[number], outs
        )
    return tuple(outs)


def solution(mesh):
    return jax.shard_map(
        per_device,
        mesh=mesh,
        in_specs=(P("sub", "vox"), P("sub", None), P("vox"), P()),
        out_specs=(P(None, "vox"), P("sub", "vox")),
        check_vma=False,
    )
```

```python
import functools

import jax
import jax.numpy as jnp
from jax import lax
from jax.experimental import pallas as pl
from jax.experimental.pallas import tpu as pltpu
from jax.sharding import PartitionSpec as P


COVARS = 64
PX = 8
PY = 8
GZ = 32
NPY = 8
QUANT = 20
LANES = 128

LAYER = PY * GZ
HALVES = LAYER // LANES
PER_TILE = LANES // GZ
CHUNKS = ((PX - 1, 0), (1, 2), (3, 4), (5, 6))
EARLY = 2
GROUP = 8
FINISH = ((0, 1), (2, 3))
ROWS = 256
LIMIT = 16 << 20

penalty_fit = 1.0
penalty_tv = 1.0
tv_weight = 0.05
huber_width = 0.02
CLIP_TV = tv_weight / penalty_tv
KAPPA = CLIP_TV / (huber_width + CLIP_TV)

F32 = jnp.float32
BF16 = jnp.bfloat16

VMEM = pl.BlockSpec(memory_space=pltpu.VMEM)
SMEM = pl.BlockSpec(memory_space=pltpu.SMEM)
ANY = pl.BlockSpec(memory_space=pl.ANY)
HBM = pl.BlockSpec(memory_space=pltpu.HBM)


def moved(block, axis, distance):
    size = lax.axis_size(axis)
    route = [((i - distance) % size, i) for i in range(size)]
    return lax.ppermute(block, axis, route)


def others_sum(block, axis):
    received = moved(block, axis, 1)
    for distance in range(2, lax.axis_size(axis)):
        received = received + moved(block, axis, distance)
    return received


def windows(layers):
    runs = []
    for place, layer in enumerate(layers):
        if runs and runs[-1][0] + runs[-1][2] == layer * LAYER:
            runs[-1][2] += LAYER
        else:
            runs.append([layer * LAYER, place * LAYER, LAYER])
    return runs


def dot(a, b):
    return jnp.dot(a, b, preferred_element_type=F32)


def halves(value):
    high = value.astype(BF16)
    return high, (value - high.astype(F32)).astype(BF16)


def columns_of(ref, layers, rows=slice(None)):
    return jnp.concatenate([ref[rows, first : first + width] for first, _, width in windows(layers)], 1)


def copies(source, target, sems, layers, into_chunk):
    plan = []
    for block in range(source.shape[0] // ROWS):
        rows = pl.ds(block * ROWS, ROWS)
        row = []
        for number, (first, place, width) in enumerate(windows(layers)):
            far, near = (rows, pl.ds(first, width)), (rows, pl.ds(place, width))
            src, dst = (far, near) if into_chunk else (near, far)
            row.append(pltpu.make_async_copy(source.at[src], target.at[dst], sems.at[block, number]))
        plan.append(row)
    return plan


def start(row):
    for copy in row:
        copy.start()


def wait(row):
    for copy in row:
        copy.wait()


def call(kernel, out_shape, in_specs, out_specs, scratch, flops, args, aliases=None):
    return pl.pallas_call(
        kernel,
        out_shape=out_shape,
        in_specs=in_specs,
        out_specs=out_specs,
        scratch_shapes=scratch,
        input_output_aliases=aliases or {},
        cost_estimate=pl.CostEstimate(flops=flops, bytes_accessed=4 << 20, transcendentals=0),
        compiler_params=pltpu.CompilerParams(vmem_limit_bytes=LIMIT),
    )(*args)


def sds(*shape, dtype=F32):
    return jax.ShapeDtypeStruct(shape, dtype)


def prepare_kernel(tau, place, cov, xt, xe, gram, setup):
    row = lax.broadcasted_iota(jnp.int32, setup.shape, 0)
    quantile = jnp.full(setup.shape, tau[0], jnp.int32).astype(F32) / QUANT
    pencil_y = jnp.full(setup.shape, place[0], jnp.int32)
    keep_prev = jnp.where(pencil_y > 0, 1.0, 0.0)
    keep_next = jnp.where(pencil_y < NPY - 1, 1.0, 0.0)
    setup[...] = jnp.where(row == 0, quantile, jnp.where(row == 1, keep_prev, keep_next))
    high, low = halves(cov[...])
    both = jnp.concatenate([high, low], 0)
    xt[...] = both
    turned = both.astype(F32).T.astype(BF16)
    xe[...] = jnp.concatenate([turned, turned], 1)
    summed = dot(both, turned)
    summed = summed[:COVARS] + summed[COVARS:]
    gram[...] = summed + pltpu.roll(summed, COVARS, 1)


def prepare(tau, place, cov):
    rows = cov.shape[1]
    out = (sds(2 * COVARS, rows, dtype=BF16), sds(rows, 4 * COVARS, dtype=BF16), sds(COVARS, LANES), sds(8, LANES))
    return call(prepare_kernel, out, [SMEM, SMEM, VMEM], (VMEM,) * 4, [], 1 << 24, (tau, place, cov))


def first_kernel(layers, opening, *refs):
    obs, xt, *gram, part = refs
    width = len(layers) * LAYER
    if opening:
        part[:, width:] = gram[0][...]
    total = None
    for block in range(obs.shape[0] // ROWS):
        rows = slice(block * ROWS, (block + 1) * ROWS)
        high, low = halves(columns_of(obs, layers, rows))
        term = dot(xt[:, rows], high) + dot(xt[:, rows], low)
        total = term if total is None else total + term
    part[:, :width] = total[:COVARS] + total[COVARS:]


def first_stage(layers, args, opening):
    rows, width = args[0].shape[0], len(layers) * LAYER
    out = sds(COVARS, width + (LANES if opening else 0))
    flops = 2 * rows * 2 * COVARS * 2 * width
    kernel = functools.partial(first_kernel, layers, opening)
    return call(kernel, out, [VMEM] * len(args), VMEM, [], flops, args)


def packed_rows(chunks, lane):
    at = lax.broadcasted_iota(jnp.int32, (COVARS, LANES), 1) // GZ
    tiles = []
    for tile in range(PX // PER_TILE):
        built = None
        for place in range(PER_TILE):
            layer = tile * PER_TILE + place
            number = next(n for n, layers in enumerate(CHUNKS) if layer in layers)
            first = CHUNKS[number].index(layer) * LAYER + lane * GZ
            base = first // LANES * LANES
            piece = chunks[number][:, base : base + LANES]
            shift = (place * GZ - (first - base)) % LANES
            piece = pltpu.roll(piece, shift, 1) if shift else piece
            built = piece if built is None else jnp.where(at == place, piece, built)
        tiles.append(built)
    return jnp.concatenate(tiles, 1)


def updated(stage, eta, mask, layers, own, got, base, grad):
    width = len(layers) * LAYER
    scale = eta * columns_of(mask, layers).astype(F32)
    summed = penalty_fit * (own[:, :width] + got[:, :width])
    if stage == 1:
        return scale * summed, None
    now = base[...] + (2.0 * scale) * summed - (eta * penalty_tv) * grad[...]
    return now, now - scale * summed


def coef_kernel(stage, *refs):
    refs = list(refs)
    take = lambda: refs.pop(0)
    mask, eta = take(), take()[0:1, 0:1]
    sums = [[take() for _ in range(2 if stage == 1 else 4)] for _ in CHUNKS[EARLY:]]
    order = [take() for _ in range(EARLY)]
    for layers, (own, got, *old) in zip(CHUNKS[EARLY:], sums):
        coef = take()
        order.append(coef)
        now, rest = updated(stage, eta, mask, layers, own, got, *(old or (None, None)))
        coef[...] = now
        if stage == 2:
            take()[...] = rest
    heads, tails = refs
    heads[...] = packed_rows(order, 0)
    tails[...] = packed_rows(order, PY - 1)


def coef_stage(stage, mask, eta, sums, earlier):
    args = [mask, eta] + [a for group in sums for a in group] + list(earlier)
    out = []
    for layers in CHUNKS[EARLY:]:
        out += [sds(COVARS, len(layers) * LAYER)] * stage
    out += [sds(COVARS, PX * GZ)] * 2
    kernel = functools.partial(coef_kernel, stage)
    results = list(call(kernel, tuple(out), [VMEM] * len(args), (VMEM,) * len(out), [], 1 << 20, args))
    return results[:-2:stage], results[1:-2:2] if stage == 2 else [], *results[-2:]


def step_kernel(layers, stage, opening, update, *refs):
    refs = list(refs)
    take = lambda: refs.pop(0)
    setup = take()
    if update:
        mask, own, got = take(), take(), take()
        eta = None if opening else take()[0:1, 0:1]
        base, grad = (take(), take()) if stage > 1 else (None, None)
    else:
        given = take()
    xe, xt, y = [take() for _ in range(3)]
    state = take() if stage > 1 else None
    if update:
        coef = take()
        eta_out = take() if opening else None
        carry = take() if stage > 1 else None
        sides = take() if PX - 1 in layers else None
    part, state_out, bext = [take() for _ in range(3)]

    width = len(layers) * LAYER
    if update:
        if opening:
            gram = jnp.abs(own[:, width:] + got[:, width:])
            first_half = lax.broadcasted_iota(jnp.int32, gram.shape, 1) < COVARS
            bound = jnp.max(jnp.sum(jnp.where(first_half, gram, 0.0), 0, keepdims=True), 1, keepdims=True)
            eta = 1.0 / (penalty_fit * bound + 12.0 * penalty_tv)
            eta_out[...] = jnp.broadcast_to(eta, eta_out.shape)
        now, rest = updated(stage, eta, mask, layers, own, got, base, grad)
        coef[...] = now
        if stage > 1:
            carry[...] = rest
        if sides is not None:
            for spot, layer in enumerate((PX - 1, 0)):
                first = layers.index(layer) * LAYER
                sides[:, spot * LAYER : (spot + 1) * LAYER] = now[:, first : first + LAYER]
    else:
        now = given[...]
    quantile = jnp.broadcast_to(setup[0:1, 0:1], (1, width))
    lower, upper = (quantile - 1.0) / penalty_fit, quantile / penalty_fit
    high, low = halves(now)
    bext[...] = jnp.concatenate([high, high, low, low], 0)
    total = None
    blocks = y.shape[0] // ROWS
    following = dot(xe[:ROWS, :], bext[...])
    for block in range(blocks):
        rows = slice(block * ROWS, (block + 1) * ROWS)
        fit = following
        if block + 1 < blocks:
            following = dot(xe[(block + 1) * ROWS : (block + 2) * ROWS, :], bext[...])
        image = columns_of(y, layers, rows)
        dual = jnp.clip((image if stage == 1 else state[rows, :]) - fit, lower, upper)
        state_out[rows, :] = image + dual
        high, low = halves(dual)
        term = dot(xt[:, rows], high) + dot(xt[:, rows], low)
        total = term if total is None else total + term
    part[...] = total[:COVARS] + total[COVARS:]


def step_stage(layers, stage, opening, setup, head, heavy):
    width, rows = len(layers) * LAYER, heavy[2].shape[0]
    update = len(head) > 1
    args = [setup] + [a for a in head + heavy if a is not None]
    specs = [VMEM] * len(args)
    out = []
    if update:
        out.append(sds(COVARS, width))
        out += [sds(8, LANES)] if opening else []
        out += [sds(COVARS, width)] if stage > 1 else []
        out += [sds(COVARS, 2 * LAYER)] if PX - 1 in layers else []
    out += [sds(COVARS, width), sds(rows, width)]
    scratch = [pltpu.VMEM((4 * COVARS, width), BF16)]
    kernel = functools.partial(step_kernel, layers, stage, opening, update)
    flops = 2 * rows * width * 2 * (2 * COVARS + 2 * COVARS)
    return list(call(kernel, tuple(out), specs, (VMEM,) * len(out), scratch, flops, args))


def tv_kernel(passes, edge, *refs):
    refs = list(refs)
    fields = []
    for _ in range(passes):
        chunks = [refs.pop(0) for _ in CHUNKS]
        from_left, from_right = refs.pop(0), refs.pop(0)
        heads, tails, before, after = [refs.pop(0) for _ in range(4)]
        fields.append((chunks, from_left, from_right, heads, tails, before, after))
    outs = refs
    place_of = {layer: (n, c.index(layer)) for n, c in enumerate(CHUNKS) for layer in c}
    lane = lax.broadcasted_iota(jnp.int32, (GROUP, LANES), 1)

    def one_group(group, carry):
        rows = pl.ds(pl.multiple_of(group * GROUP, GROUP), GROUP)
        keep_prev, keep_y = edge[1:2, :], edge[2:3, :]

        def tile(field, layer, half):
            chunks, from_left, from_right = field[:3]
            if layer < 0:
                return from_left[rows, half * LANES : (half + 1) * LANES]
            if layer == PX:
                return from_right[rows, LAYER + half * LANES : LAYER + (half + 1) * LANES]
            number, place = place_of[layer]
            first = place * LAYER + half * LANES
            return chunks[number][rows, first : first + LANES]

        def dual_of(steps):
            q = None
            for step in steps[:-1]:
                q = jnp.clip((step if q is None else step + q) * KAPPA, -CLIP_TV, CLIP_TV)
            step = steps[-1] if q is None else steps[-1] + q
            twice = jnp.clip(step * (2.0 * KAPPA), -2.0 * CLIP_TV, 2.0 * CLIP_TV)
            return twice if q is None else twice - q

        def dual_x(layer, half):
            return dual_of([tile(f, layer + 1, half) - tile(f, layer, half) for f in fields])

        def dual_z(layer, half):
            steps = []
            for f in fields:
                now = tile(f, layer, half)
                steps.append(jnp.where(lane % GZ == GZ - 1, 0.0, pltpu.roll(now, LANES - 1, 1) - now))
            return dual_of(steps)

        def dual_y(layer, half):
            steps = []
            group_at, spot = layer // PER_TILE, layer % PER_TILE
            for f in fields:
                now = tile(f, layer, half)
                if half + 1 < HALVES:
                    after = pltpu.roll(tile(f, layer, half + 1), LANES - GZ, 1)
                else:
                    after = f[6][rows, group_at * LANES : (group_at + 1) * LANES]
                    shift = (LANES - GZ - spot * GZ) % LANES
                    after = pltpu.roll(after, shift, 1) if shift else after
                following = jnp.where(lane < LANES - GZ, pltpu.roll(now, LANES - GZ, 1), after)
                step = following - now
                if half + 1 == HALVES:
                    step = step * jnp.where(lane < LANES - GZ, 1.0, keep_y)
                steps.append(step)
            return dual_of(steps)

        edge_duals = []
        for group_at in range(PX // PER_TILE):
            at = slice(group_at * LANES, (group_at + 1) * LANES)
            edge_duals.append(dual_of([(f[3][rows, at] - f[5][rows, at]) * keep_prev for f in fields]))

        before_x = [dual_x(-1, half) for half in range(HALVES)]
        for layer in range(PX):
            number, place = place_of[layer]
            group_at, spot = layer // PER_TILE, layer % PER_TILE
            shift = (LANES - spot * GZ) % LANES
            before_y = pltpu.roll(edge_duals[group_at], shift, 1) if shift else edge_duals[group_at]
            for half in range(HALVES):
                x_now = dual_x(layer, half)
                y_now = dual_y(layer, half)
                z_now = dual_z(layer, half)
                rolled = pltpu.roll(y_now, GZ, 1)
                summed = before_x[half] - x_now
                summed = summed + (jnp.where(lane < GZ, before_y, rolled) - y_now)
                summed = summed + (pltpu.roll(z_now, 1, 1) - z_now)
                first = place * LAYER + half * LANES
                outs[number][rows, first : first + LANES] = summed
                before_x[half] = x_now
                before_y = rolled
        return carry

    lax.fori_loop(0, COVARS // GROUP, one_group, 0)


def tv_stage(edge, fields):
    args, specs = [edge], [VMEM]
    for chunks, *rest in fields:
        args += list(chunks) + rest
        specs += [VMEM] * (len(chunks) + len(rest))
    out = tuple(sds(COVARS, len(c) * LAYER) for c in CHUNKS)

    def kernel(edge_ref, *refs):
        tv_kernel(len(fields), edge_ref, *refs)

    flops = len(fields) * 60 * COVARS * PX * LAYER * 64
    return call(kernel, out, specs, (VMEM,) * len(out), [], flops, args)


def last_kernel(group, first, *refs):
    refs = list(refs)
    take = lambda: refs.pop(0)
    setup, mask, eta, xe = [take() for _ in range(4)]
    chunks = [[take() for _ in range(5)] for _ in group]
    if not first:
        take(), take()
    coef_out, res_out = take(), take()
    step = eta[0:1, 0:1]
    plan = []
    for layers, (own, got, base, grad, state) in zip(group, chunks):
        bext, rbuf, rsems, cbuf, csems = [take() for _ in range(5)]
        width = len(layers) * LAYER
        kept = columns_of(mask, layers).astype(F32)
        quantile = jnp.broadcast_to(setup[0:1, 0:1], (1, width))
        lower, upper = (quantile - 1.0) / penalty_fit, quantile / penalty_fit
        summed = penalty_fit * (own[:, :width] + got[:, :width])
        now = base[...] + (2.0 * step * kept) * summed - (step * penalty_tv) * grad[...]
        cbuf[...] = now
        coef_stores = []
        for number, (at, place, span) in enumerate(windows(layers)):
            coef_stores.append(
                pltpu.make_async_copy(cbuf.at[:, pl.ds(place, span)], coef_out.at[:, pl.ds(at, span)], csems.at[number])
            )
        start(coef_stores)
        high, low = halves(now)
        bext[...] = jnp.concatenate([high, high, low, low], 0)
        stores = copies(rbuf, res_out, rsems, layers, False)
        for block, row in enumerate(stores):
            rows = slice(block * ROWS, (block + 1) * ROWS)
            target = state[rows, :] - dot(xe[rows, :], bext[...])
            rbuf[rows, :] = kept * (target - jnp.clip(target, lower, upper))
            start(row)
        plan += [coef_stores] + stores
    for row in plan:
        wait(row)


def last_stage(group, pencil, setup, mask, eta, xe, chunks, outs):
    rows = xe.shape[0]
    args, specs = [setup, mask, eta, xe], [VMEM] * 4
    for chunk in chunks:
        args, specs = args + list(chunk), specs + [VMEM] * len(chunk)
    aliases = {}
    if outs is not None:
        aliases = {len(args): 0, len(args) + 1: 1}
        args, specs = args + list(outs), specs + [HBM, HBM]
    scratch, flops = [], 0
    for layers in group:
        width, runs = len(layers) * LAYER, len(windows(layers))
        scratch += [
            pltpu.VMEM((4 * COVARS, width), BF16),
            pltpu.VMEM((rows, width), F32),
            pltpu.SemaphoreType.DMA((rows // ROWS, runs)),
            pltpu.VMEM((COVARS, width), F32),
            pltpu.SemaphoreType.DMA((runs,)),
        ]
        flops += 2 * rows * width * 4 * COVARS * 2
    out = (sds(COVARS, pencil), sds(rows, pencil))
    kernel = functools.partial(last_kernel, group, outs is None)
    return call(kernel, out, specs, (HBM, HBM), scratch, flops, args, aliases)


def neighbours_x(chunk):
    size = lax.axis_size("vox")
    before = moved(chunk, "vox", NPY)
    after = before if (2 * NPY) % size == 0 else moved(chunk, "vox", -NPY)
    return before, after


def per_device(observed, covariates, voxel_mask, tau_index):
    pencils = lax.axis_size("vox")
    pencil_y = (lax.axis_index("vox") + NPY // 2) % pencils % NPY
    mask = voxel_mask.reshape(1, -1)

    parts = []
    xt, xe, gram, setup = prepare(tau_index, pencil_y.reshape(1), covariates.T)
    for number, layers in enumerate(CHUNKS):
        args = [observed, xt] + ([] if number else [gram])
        part = first_stage(layers, args, number == 0)
        parts.append((part, others_sum(part, "sub")))

    eta, base, grad, states, fields = None, None, None, [None] * len(CHUNKS), []
    for stage in (1, 2):
        coefs, carries, new_parts, new_states = [], [], [], []
        for number, layers in enumerate(CHUNKS):
            opening = eta is None
            update = [mask, *parts[number], eta, base[number] if base else None, grad[number] if grad else None]
            heavy = [xe, xt, observed, states[number]]
            if number < EARLY:
                results = step_stage(layers, stage, opening, setup, update, heavy)
                coefs.append(results.pop(0))
                if opening:
                    eta = results.pop(0)
                if stage == 2:
                    carries.append(results.pop(0))
                if number == 0:
                    from_left, from_right = neighbours_x(results.pop(0))
            if number == EARLY:
                rest = range(EARLY, len(CHUNKS))
                sums = [parts[n] + ((base[n], grad[n]) if stage == 2 else ()) for n in rest]
                more, more_carries, heads, tails = coef_stage(stage, mask, eta, sums, coefs)
                coefs, carries = coefs + more, carries + more_carries
                before = moved(tails, "vox", 1)
                after = moved(heads, "vox", -1)
            if number >= EARLY:
                results = step_stage(layers, stage, False, setup, [coefs[number]], heavy)
            part, state = results
            new_states.append(state)
            new_parts.append((part, others_sum(part, "sub")))
        fields.append((coefs, from_left, from_right, heads, tails, before, after))
        grad = tv_stage(setup, fields)
        base = coefs if stage == 1 else carries
        parts, states = new_parts, new_states

    outs = None
    for members in FINISH:
        chunks = [(*parts[n], base[n], grad[n], states[n]) for n in members]
        group = tuple(CHUNKS[n] for n in members)
        outs = last_stage(group, observed.shape[1], setup, mask, eta, xe, chunks, outs)
    return tuple(outs)


def solution(mesh):
    return jax.shard_map(
        per_device,
        mesh=mesh,
        in_specs=(P("sub", "vox"), P("sub", None), P("vox"), P()),
        out_specs=(P(None, "vox"), P("sub", "vox")),
        check_vma=False,
    )
```

```python
import functools

import jax
import jax.numpy as jnp
from jax import lax
from jax.experimental import pallas as pl
from jax.experimental.pallas import tpu as pltpu
from jax.sharding import PartitionSpec as P


COVARS = 64
PX = 8
PY = 8
GZ = 32
NPY = 8
QUANT = 20
LANES = 128

LAYER = PY * GZ
HALVES = LAYER // LANES
PER_TILE = LANES // GZ
CHUNKS = ((PX - 1, 0), (1, 2), (3, 4), (5, 6))
EARLY = 2
GROUP = 8
FINISH = ((0, 1, 2, 3),)
ROWS = 256
LIMIT = 16 << 20

penalty_fit = 1.0
penalty_tv = 1.0
tv_weight = 0.05
huber_width = 0.02
CLIP_TV = tv_weight / penalty_tv
KAPPA = CLIP_TV / (huber_width + CLIP_TV)

F32 = jnp.float32
BF16 = jnp.bfloat16

VMEM = pl.BlockSpec(memory_space=pltpu.VMEM)
SMEM = pl.BlockSpec(memory_space=pltpu.SMEM)
ANY = pl.BlockSpec(memory_space=pl.ANY)
HBM = pl.BlockSpec(memory_space=pltpu.HBM)


def moved(block, axis, distance):
    size = lax.axis_size(axis)
    route = [((i - distance) % size, i) for i in range(size)]
    return lax.ppermute(block, axis, route)


def others_sum(block, axis):
    received = moved(block, axis, 1)
    for distance in range(2, lax.axis_size(axis)):
        received = received + moved(block, axis, distance)
    return received


def windows(layers):
    runs = []
    for place, layer in enumerate(layers):
        if runs and runs[-1][0] + runs[-1][2] == layer * LAYER:
            runs[-1][2] += LAYER
        else:
            runs.append([layer * LAYER, place * LAYER, LAYER])
    return runs


def dot(a, b):
    return jnp.dot(a, b, preferred_element_type=F32)


def halves(value):
    high = value.astype(BF16)
    return high, (value - high.astype(F32)).astype(BF16)


def columns_of(ref, layers, rows=slice(None)):
    return jnp.concatenate([ref[rows, first : first + width] for first, _, width in windows(layers)], 1)


def copies(source, target, sems, layers, into_chunk):
    plan = []
    for block in range(source.shape[0] // ROWS):
        rows = pl.ds(block * ROWS, ROWS)
        row = []
        for number, (first, place, width) in enumerate(windows(layers)):
            far, near = (rows, pl.ds(first, width)), (rows, pl.ds(place, width))
            src, dst = (far, near) if into_chunk else (near, far)
            row.append(pltpu.make_async_copy(source.at[src], target.at[dst], sems.at[block, number]))
        plan.append(row)
    return plan


def start(row):
    for copy in row:
        copy.start()


def wait(row):
    for copy in row:
        copy.wait()


def call(kernel, out_shape, in_specs, out_specs, scratch, flops, args, aliases=None):
    return pl.pallas_call(
        kernel,
        out_shape=out_shape,
        in_specs=in_specs,
        out_specs=out_specs,
        scratch_shapes=scratch,
        input_output_aliases=aliases or {},
        cost_estimate=pl.CostEstimate(flops=flops, bytes_accessed=4 << 20, transcendentals=0),
        compiler_params=pltpu.CompilerParams(vmem_limit_bytes=LIMIT),
    )(*args)


def sds(*shape, dtype=F32):
    return jax.ShapeDtypeStruct(shape, dtype)


def set_up(tau, place, setup):
    row = lax.broadcasted_iota(jnp.int32, setup.shape, 0)
    quantile = jnp.full(setup.shape, tau[0], jnp.int32).astype(F32) / QUANT
    pencil_y = jnp.full(setup.shape, place[0], jnp.int32)
    keep_prev = jnp.where(pencil_y > 0, 1.0, 0.0)
    keep_next = jnp.where(pencil_y < NPY - 1, 1.0, 0.0)
    setup[...] = jnp.where(row == 0, quantile, jnp.where(row == 1, keep_prev, keep_next))


def opening_kernel(layers, tau, place, cov, far, part, xt, setup, cbuf, csem, ybuf, sems):
    width = len(layers) * LAYER
    fetch = pltpu.make_async_copy(cov, cbuf, csem)
    fetch.start()
    loads = copies(far, ybuf, sems, layers, True)
    for row in loads:
        start(row)
    set_up(tau, place, setup)
    fetch.wait()
    high, low = halves(cbuf[...])
    xt[...] = jnp.concatenate([high, low], 0)
    gram = lax.dot_general(xt[...], xt[...], (((1,), (1,)), ((), ())), preferred_element_type=F32)
    gram = gram[:COVARS] + gram[COVARS:]
    part[:, width:] = gram + pltpu.roll(gram, COVARS, 1)
    total = None
    for block, row in enumerate(loads):
        wait(row)
        rows = slice(block * ROWS, (block + 1) * ROWS)
        high, low = halves(ybuf[rows, :])
        term = dot(xt[:, rows], high) + dot(xt[:, rows], low)
        total = term if total is None else total + term
    part[:, :width] = total[:COVARS] + total[COVARS:]


def opening_stage(layers, tau, place, cov, far):
    rows, width = far.shape[0], len(layers) * LAYER
    out = (sds(COVARS, width + LANES), sds(2 * COVARS, rows, dtype=BF16), sds(8, LANES))
    scratch = [
        pltpu.VMEM(cov.shape, F32),
        pltpu.SemaphoreType.DMA,
        pltpu.VMEM((rows, width), F32),
        pltpu.SemaphoreType.DMA((rows // ROWS, len(windows(layers)))),
    ]
    flops = 2 * rows * 2 * COVARS * 2 * width
    kernel = functools.partial(opening_kernel, layers)
    return call(kernel, out, [SMEM, SMEM, HBM, HBM], (VMEM,) * 3, scratch, flops, (tau, place, cov, far))


def first_kernel(layers, turn, obs, xt, part, *xe):
    total = None
    for block in range(obs.shape[0] // ROWS):
        rows = slice(block * ROWS, (block + 1) * ROWS)
        high, low = halves(columns_of(obs, layers, rows))
        term = dot(xt[:, rows], high) + dot(xt[:, rows], low)
        total = term if total is None else total + term
    part[...] = total[:COVARS] + total[COVARS:]
    if turn:
        turned = xt[...].astype(F32).T.astype(BF16)
        xe[0][...] = jnp.concatenate([turned, turned], 1)


def first_stage(layers, obs, xt, turn):
    rows, width = obs.shape[0], len(layers) * LAYER
    out = (sds(COVARS, width),) + ((sds(rows, 4 * COVARS, dtype=BF16),) if turn else ())
    flops = 2 * rows * 2 * COVARS * 2 * width
    kernel = functools.partial(first_kernel, layers, turn)
    return call(kernel, out, [VMEM, VMEM], (VMEM,) * len(out), [], flops, (obs, xt))


def packed_rows(chunks, lane):
    at = lax.broadcasted_iota(jnp.int32, (COVARS, LANES), 1) // GZ
    tiles = []
    for tile in range(PX // PER_TILE):
        built = None
        for place in range(PER_TILE):
            layer = tile * PER_TILE + place
            number = next(n for n, layers in enumerate(CHUNKS) if layer in layers)
            first = CHUNKS[number].index(layer) * LAYER + lane * GZ
            base = first // LANES * LANES
            piece = chunks[number][:, base : base + LANES]
            shift = (place * GZ - (first - base)) % LANES
            piece = pltpu.roll(piece, shift, 1) if shift else piece
            built = piece if built is None else jnp.where(at == place, piece, built)
        tiles.append(built)
    return jnp.concatenate(tiles, 1)


def updated(stage, eta, mask, layers, own, got, base, grad):
    width = len(layers) * LAYER
    scale = eta * columns_of(mask, layers).astype(F32)
    summed = penalty_fit * (own[:, :width] + got[:, :width])
    if stage == 1:
        return scale * summed, None
    now = base[...] + (2.0 * scale) * summed - (eta * penalty_tv) * grad[...]
    return now, now - scale * summed


def coef_kernel(stage, *refs):
    refs = list(refs)
    take = lambda: refs.pop(0)
    mask, eta = take(), take()[0:1, 0:1]
    sums = [[take() for _ in range(2 if stage == 1 else 4)] for _ in CHUNKS[EARLY:]]
    order = [take() for _ in range(EARLY)]
    for layers, (own, got, *old) in zip(CHUNKS[EARLY:], sums):
        coef = take()
        order.append(coef)
        now, rest = updated(stage, eta, mask, layers, own, got, *(old or (None, None)))
        coef[...] = now
        if stage == 2:
            take()[...] = rest
    heads, tails = refs
    heads[...] = packed_rows(order, 0)
    tails[...] = packed_rows(order, PY - 1)


def coef_stage(stage, mask, eta, sums, earlier):
    args = [mask, eta] + [a for group in sums for a in group] + list(earlier)
    out = []
    for layers in CHUNKS[EARLY:]:
        out += [sds(COVARS, len(layers) * LAYER)] * stage
    out += [sds(COVARS, PX * GZ)] * 2
    kernel = functools.partial(coef_kernel, stage)
    results = list(call(kernel, tuple(out), [VMEM] * len(args), (VMEM,) * len(out), [], 1 << 20, args))
    return results[:-2:stage], results[1:-2:2] if stage == 2 else [], *results[-2:]


def step_kernel(layers, stage, opening, update, *refs):
    refs = list(refs)
    take = lambda: refs.pop(0)
    setup = take()
    if update:
        mask, own, got = take(), take(), take()
        eta = None if opening else take()[0:1, 0:1]
        base, grad = (take(), take()) if stage > 1 else (None, None)
    else:
        given = take()
    xe, xt, y = [take() for _ in range(3)]
    state = take() if stage > 1 else None
    if update:
        coef = take()
        eta_out = take() if opening else None
        carry = take() if stage > 1 else None
        sides = take() if PX - 1 in layers else None
    part, state_out, bext = [take() for _ in range(3)]

    width = len(layers) * LAYER
    if update:
        if opening:
            gram = jnp.abs(own[:, width:] + got[:, width:])
            first_half = lax.broadcasted_iota(jnp.int32, gram.shape, 1) < COVARS
            bound = jnp.max(jnp.sum(jnp.where(first_half, gram, 0.0), 0, keepdims=True), 1, keepdims=True)
            eta = 1.0 / (penalty_fit * bound + 12.0 * penalty_tv)
            eta_out[...] = jnp.broadcast_to(eta, eta_out.shape)
        now, rest = updated(stage, eta, mask, layers, own, got, base, grad)
        coef[...] = now
        if stage > 1:
            carry[...] = rest
        if sides is not None:
            for spot, layer in enumerate((PX - 1, 0)):
                first = layers.index(layer) * LAYER
                sides[:, spot * LAYER : (spot + 1) * LAYER] = now[:, first : first + LAYER]
    else:
        now = given[...]
    quantile = jnp.broadcast_to(setup[0:1, 0:1], (1, width))
    lower, upper = (quantile - 1.0) / penalty_fit, quantile / penalty_fit
    high, low = halves(now)
    bext[...] = jnp.concatenate([high, high, low, low], 0)
    total = None
    blocks = y.shape[0] // ROWS
    following = dot(xe[:ROWS, :], bext[...])
    for block in range(blocks):
        rows = slice(block * ROWS, (block + 1) * ROWS)
        fit = following
        if block + 1 < blocks:
            following = dot(xe[(block + 1) * ROWS : (block + 2) * ROWS, :], bext[...])
        image = columns_of(y, layers, rows)
        dual = jnp.clip((image if stage == 1 else state[rows, :]) - fit, lower, upper)
        state_out[rows, :] = image + dual
        high, low = halves(dual)
        term = dot(xt[:, rows], high) + dot(xt[:, rows], low)
        total = term if total is None else total + term
    part[...] = total[:COVARS] + total[COVARS:]


def step_stage(layers, stage, opening, setup, head, heavy):
    width, rows = len(layers) * LAYER, heavy[2].shape[0]
    update = len(head) > 1
    args = [setup] + [a for a in head + heavy if a is not None]
    specs = [VMEM] * len(args)
    out = []
    if update:
        out.append(sds(COVARS, width))
        out += [sds(8, LANES)] if opening else []
        out += [sds(COVARS, width)] if stage > 1 else []
        out += [sds(COVARS, 2 * LAYER)] if PX - 1 in layers else []
    out += [sds(COVARS, width), sds(rows, width)]
    scratch = [pltpu.VMEM((4 * COVARS, width), BF16)]
    kernel = functools.partial(step_kernel, layers, stage, opening, update)
    flops = 2 * rows * width * 2 * (2 * COVARS + 2 * COVARS)
    return list(call(kernel, tuple(out), specs, (VMEM,) * len(out), scratch, flops, args))


def tv_kernel(passes, edge, *refs):
    refs = list(refs)
    fields = []
    for _ in range(passes):
        chunks = [refs.pop(0) for _ in CHUNKS]
        from_left, from_right = refs.pop(0), refs.pop(0)
        heads, tails, before, after = [refs.pop(0) for _ in range(4)]
        fields.append((chunks, from_left, from_right, heads, tails, before, after))
    outs = refs
    place_of = {layer: (n, c.index(layer)) for n, c in enumerate(CHUNKS) for layer in c}
    lane = lax.broadcasted_iota(jnp.int32, (GROUP, LANES), 1)

    def one_group(group, carry):
        rows = pl.ds(pl.multiple_of(group * GROUP, GROUP), GROUP)
        keep_prev, keep_y = edge[1:2, :], edge[2:3, :]

        def tile(field, layer, half):
            chunks, from_left, from_right = field[:3]
            if layer < 0:
                return from_left[rows, half * LANES : (half + 1) * LANES]
            if layer == PX:
                return from_right[rows, LAYER + half * LANES : LAYER + (half + 1) * LANES]
            number, place = place_of[layer]
            first = place * LAYER + half * LANES
            return chunks[number][rows, first : first + LANES]

        def dual_of(steps):
            q = None
            for step in steps[:-1]:
                q = jnp.clip((step if q is None else step + q) * KAPPA, -CLIP_TV, CLIP_TV)
            step = steps[-1] if q is None else steps[-1] + q
            twice = jnp.clip(step * (2.0 * KAPPA), -2.0 * CLIP_TV, 2.0 * CLIP_TV)
            return twice if q is None else twice - q

        def dual_x(layer, half):
            return dual_of([tile(f, layer + 1, half) - tile(f, layer, half) for f in fields])

        def dual_z(layer, half):
            steps = []
            for f in fields:
                now = tile(f, layer, half)
                steps.append(jnp.where(lane % GZ == GZ - 1, 0.0, pltpu.roll(now, LANES - 1, 1) - now))
            return dual_of(steps)

        def dual_y(layer, half):
            steps = []
            group_at, spot = layer // PER_TILE, layer % PER_TILE
            for f in fields:
                now = tile(f, layer, half)
                if half + 1 < HALVES:
                    after = pltpu.roll(tile(f, layer, half + 1), LANES - GZ, 1)
                else:
                    after = f[6][rows, group_at * LANES : (group_at + 1) * LANES]
                    shift = (LANES - GZ - spot * GZ) % LANES
                    after = pltpu.roll(after, shift, 1) if shift else after
                following = jnp.where(lane < LANES - GZ, pltpu.roll(now, LANES - GZ, 1), after)
                step = following - now
                if half + 1 == HALVES:
                    step = step * jnp.where(lane < LANES - GZ, 1.0, keep_y)
                steps.append(step)
            return dual_of(steps)

        edge_duals = []
        for group_at in range(PX // PER_TILE):
            at = slice(group_at * LANES, (group_at + 1) * LANES)
            edge_duals.append(dual_of([(f[3][rows, at] - f[5][rows, at]) * keep_prev for f in fields]))

        before_x = [dual_x(-1, half) for half in range(HALVES)]
        for layer in range(PX):
            number, place = place_of[layer]
            group_at, spot = layer // PER_TILE, layer % PER_TILE
            shift = (LANES - spot * GZ) % LANES
            before_y = pltpu.roll(edge_duals[group_at], shift, 1) if shift else edge_duals[group_at]
            for half in range(HALVES):
                x_now = dual_x(layer, half)
                y_now = dual_y(layer, half)
                z_now = dual_z(layer, half)
                rolled = pltpu.roll(y_now, GZ, 1)
                summed = before_x[half] - x_now
                summed = summed + (jnp.where(lane < GZ, before_y, rolled) - y_now)
                summed = summed + (pltpu.roll(z_now, 1, 1) - z_now)
                first = place * LAYER + half * LANES
                outs[number][rows, first : first + LANES] = summed
                before_x[half] = x_now
                before_y = rolled
        return carry

    lax.fori_loop(0, COVARS // GROUP, one_group, 0)


def tv_stage(edge, fields):
    args, specs = [edge], [VMEM]
    for chunks, *rest in fields:
        args += list(chunks) + rest
        specs += [VMEM] * (len(chunks) + len(rest))
    out = tuple(sds(COVARS, len(c) * LAYER) for c in CHUNKS)

    def kernel(edge_ref, *refs):
        tv_kernel(len(fields), edge_ref, *refs)

    flops = len(fields) * 60 * COVARS * PX * LAYER * 64
    return call(kernel, out, specs, (VMEM,) * len(out), [], flops, args)


def last_kernel(group, first, *refs):
    refs = list(refs)
    take = lambda: refs.pop(0)
    setup, mask, eta, xe = [take() for _ in range(4)]
    chunks = [[take() for _ in range(5)] for _ in group]
    if not first:
        take(), take()
    coef_out, res_out = take(), take()
    step = eta[0:1, 0:1]
    plan = []
    for layers, (own, got, base, grad, state) in zip(group, chunks):
        bext, rbuf, rsems, cbuf, csems = [take() for _ in range(5)]
        width = len(layers) * LAYER
        kept = columns_of(mask, layers).astype(F32)
        quantile = jnp.broadcast_to(setup[0:1, 0:1], (1, width))
        lower, upper = (quantile - 1.0) / penalty_fit, quantile / penalty_fit
        summed = penalty_fit * (own[:, :width] + got[:, :width])
        now = base[...] + (2.0 * step * kept) * summed - (step * penalty_tv) * grad[...]
        cbuf[...] = now
        coef_stores = []
        for number, (at, place, span) in enumerate(windows(layers)):
            coef_stores.append(
                pltpu.make_async_copy(cbuf.at[:, pl.ds(place, span)], coef_out.at[:, pl.ds(at, span)], csems.at[number])
            )
        start(coef_stores)
        high, low = halves(now)
        bext[...] = jnp.concatenate([high, high, low, low], 0)
        stores = copies(rbuf, res_out, rsems, layers, False)
        for block, row in enumerate(stores):
            rows = slice(block * ROWS, (block + 1) * ROWS)
            target = state[rows, :] - dot(xe[rows, :], bext[...])
            rbuf[rows, :] = kept * (target - jnp.clip(target, lower, upper))
            start(row)
        plan += [coef_stores] + stores
    for row in plan:
        wait(row)


def last_stage(group, pencil, setup, mask, eta, xe, chunks, outs):
    rows = xe.shape[0]
    args, specs = [setup, mask, eta, xe], [VMEM] * 4
    for chunk in chunks:
        args, specs = args + list(chunk), specs + [VMEM] * len(chunk)
    aliases = {}
    if outs is not None:
        aliases = {len(args): 0, len(args) + 1: 1}
        args, specs = args + list(outs), specs + [HBM, HBM]
    scratch, flops = [], 0
    for layers in group:
        width, runs = len(layers) * LAYER, len(windows(layers))
        scratch += [
            pltpu.VMEM((4 * COVARS, width), BF16),
            pltpu.VMEM((rows, width), F32),
            pltpu.SemaphoreType.DMA((rows // ROWS, runs)),
            pltpu.VMEM((COVARS, width), F32),
            pltpu.SemaphoreType.DMA((runs,)),
        ]
        flops += 2 * rows * width * 4 * COVARS * 2
    out = (sds(COVARS, pencil), sds(rows, pencil))
    kernel = functools.partial(last_kernel, group, outs is None)
    return call(kernel, out, specs, (HBM, HBM), scratch, flops, args, aliases)


def neighbours_x(chunk):
    size = lax.axis_size("vox")
    before = moved(chunk, "vox", NPY)
    after = before if (2 * NPY) % size == 0 else moved(chunk, "vox", -NPY)
    return before, after


def per_device(observed, covariates, voxel_mask, tau_index):
    pencils = lax.axis_size("vox")
    pencil_y = (lax.axis_index("vox") + NPY // 2) % pencils % NPY
    mask = voxel_mask.reshape(1, -1)

    parts, more = [], []
    in_hbm = [pltpu.with_memory_space_constraint(a, pltpu.HBM) for a in (covariates.T, observed)]
    for number, layers in enumerate(CHUNKS):
        if number == 0:
            part, xt, setup = opening_stage(layers, tau_index, pencil_y.reshape(1), *in_hbm)
        else:
            part, *turned = first_stage(layers, observed, xt, number == 1)
            more += turned
        parts.append((part, others_sum(part, "sub")))
    (xe,) = more

    eta, base, grad, states, fields = None, None, None, [None] * len(CHUNKS), []
    for stage in (1, 2):
        coefs, carries, new_parts, new_states = [], [], [], []
        for number, layers in enumerate(CHUNKS):
            opening = eta is None
            update = [mask, *parts[number], eta, base[number] if base else None, grad[number] if grad else None]
            heavy = [xe, xt, observed, states[number]]
            if number < EARLY:
                results = step_stage(layers, stage, opening, setup, update, heavy)
                coefs.append(results.pop(0))
                if opening:
                    eta = results.pop(0)
                if stage == 2:
                    carries.append(results.pop(0))
                if number == 0:
                    from_left, from_right = neighbours_x(results.pop(0))
            if number == EARLY:
                rest = range(EARLY, len(CHUNKS))
                sums = [parts[n] + ((base[n], grad[n]) if stage == 2 else ()) for n in rest]
                more, more_carries, heads, tails = coef_stage(stage, mask, eta, sums, coefs)
                coefs, carries = coefs + more, carries + more_carries
                before = moved(tails, "vox", 1)
                after = moved(heads, "vox", -1)
            if number >= EARLY:
                results = step_stage(layers, stage, False, setup, [coefs[number]], heavy)
            part, state = results
            new_states.append(state)
            new_parts.append((part, others_sum(part, "sub")))
        fields.append((coefs, from_left, from_right, heads, tails, before, after))
        grad = tv_stage(setup, fields)
        base = coefs if stage == 1 else carries
        parts, states = new_parts, new_states

    outs = None
    for members in FINISH:
        chunks = [(*parts[n], base[n], grad[n], states[n]) for n in members]
        group = tuple(CHUNKS[n] for n in members)
        outs = last_stage(group, observed.shape[1], setup, mask, eta, xe, chunks, outs)
    return tuple(outs)


def solution(mesh):
    return jax.shard_map(
        per_device,
        mesh=mesh,
        in_specs=(P("sub", "vox"), P("sub", None), P("vox"), P()),
        out_specs=(P(None, "vox"), P("sub", "vox")),
        check_vma=False,
    )
```
